128 devices in a mesh: out: 8 (over x, y_lo), con: 16 (over z, y_hi, core).
Axes of the slice: x: 4, y: 4 (y_hi: 2, y_lo: 2; y = y_hi * 2 + y_lo), z: 4, core: 2. Of those that a mesh axis runs over, the one named last changes fastest.
Arguments:
- fitted_factors: bfloat16 [512, 512, 1536], P('out', 'con'), may hold values from -0.119628906 to 0.119628906
- amplitudes: bfloat16 [512, 512, 256], P(None, 'con'), may hold values from -1.796875 to 1.796875
- driver_term: float32 [4, 256, 512], P(None, None, 'out'), may hold values from -9 to 9
- occ_energy: float32 [16], replicated, may hold values from -1 to -0.5
- vir_energy: float32 [512], replicated, may hold values from 0.5 to 1.5
- window_rows: int32 [4], replicated, may hold values from 0 to 511, as said below
Outputs:
- first_update: bfloat16 [4, 256, 512], P(None, 'con', 'out')
- second_update: bfloat16 [4, 256, 512], P(None, 'con', 'out')
The draws below stay inside these ranges and needn't reach their ends.
Inputs may be any that keep to these rules, and one draw needn't show every extreme that they name: `window_rows`: the 4 entries are distinct.
All inputs are finite; a program needn't handle non-finite values.
Results may differ from the reference program's by a relative error of at most 0.006.
Values may be sent and summed in bfloat16 or wider, within the bound.
No kernel may reach another device: no remote copies, remote signals or barrier semaphores. Data moves between devices by JAX's collectives and lax.ppermute only.
A program may use at most 128 MiB of HBM per device.

```python
import jax
import jax.numpy as jnp
from jax import lax

VIRTUALS = 512
AUXILIARY = 1536
OCCUPIED = 16
WINDOW_ROWS = 4
OCC_PAIRS = 256


def draw_window_rows(key, part):
    order = jax.random.permutation(jax.random.fold_in(key, 11), VIRTUALS - 1)
    chosen = jnp.concatenate([order[:WINDOW_ROWS - 1].astype(jnp.int32), jnp.full((1,), VIRTUALS - 1, jnp.int32)])
    places = jax.random.permutation(jax.random.fold_in(key, 23), WINDOW_ROWS)
    return chosen[places].astype(jnp.int32)


def level_of(key, shape, pieces, low, high):
    gain, own = 1.0, jax.random.fold_in(key, 6)
    for position, shards_of in pieces:
        heights = jnp.exp(jax.random.uniform(jax.random.fold_in(own, position), (shards_of,), jnp.float32, low / len(pieces), high / len(pieces)))
        gain = gain * jnp.repeat(heights, shape[position] // shards_of).reshape([-1 if axis == position else 1 for axis in range(len(shape))])
    return gain


def centred(own_key, shape, deviation, bound, pieces=(), kind=jnp.bfloat16):
    array = jax.random.normal(own_key, shape, jnp.float32) * deviation
    if len(pieces) > 0:
        array = level_of(own_key, shape, pieces, -0.22, 0.18) * array
    return jnp.clip(array, min=-bound, max=bound).astype(kind)


def setup_inputs(seed: int = 0) -> dict:
    arg_keys = jax.random.split(jax.random.key(seed), 7)
    fitted_factors = centred(arg_keys[0], (VIRTUALS, VIRTUALS, AUXILIARY), ((8.0 / VIRTUALS) ** 0.5 * AUXILIARY ** -0.25), 0.119628906, ((0, 8), (1, 16)))
    amplitudes = centred(arg_keys[1], (VIRTUALS, VIRTUALS, OCC_PAIRS), 0.3, 1.796875, ((1, 16),))
    driver_term = centred(arg_keys[2], (WINDOW_ROWS, OCC_PAIRS, VIRTUALS), 1.5, 9.0, ((2, 8),), jnp.float32)
    occ_energy = jnp.clip(jax.random.uniform(arg_keys[3], (OCCUPIED,), jnp.float32, -1.0, -0.5), -1.0, -0.5)
    vir_energy = jnp.clip(jax.random.uniform(arg_keys[4], (VIRTUALS,), jnp.float32, 0.5, 1.5), 0.5, 1.5)
    window_rows = draw_window_rows(jax.random.fold_in(arg_keys[6], 71), 0)
    return {"fitted_factors": fitted_factors, "amplitudes": amplitudes, "driver_term": driver_term, "occ_energy": occ_energy, "vir_energy": vir_energy, "window_rows": window_rows}


def reference(fitted_factors, amplitudes, driver_term, occ_energy, vir_energy, window_rows):
    rows = fitted_factors[window_rows]
    width = VIRTUALS // 8
    amp_wide = amplitudes.astype(jnp.float32)

    def per_row(row):
        def per_block(index):
            part = lax.dynamic_slice_in_dim(fitted_factors, (index * width).astype(jnp.int32), width, 0)
            block = jnp.einsum("cq,bdq->cbd", row.astype(jnp.float32), part.astype(jnp.float32)).astype(jnp.bfloat16)
            ladder = jnp.einsum("cbd,cdi->ib", block.astype(jnp.float32), amp_wide)
            picked = block[window_rows]
            return ladder, picked

        ladders, picked = lax.map(per_block, jnp.arange(8, dtype=jnp.int32))
        ladder = jnp.transpose(ladders, (1, 0, 2)).reshape(OCC_PAIRS, VIRTUALS)
        picked = jnp.transpose(picked, (1, 0, 2, 3)).reshape(WINDOW_ROWS, VIRTUALS, VIRTUALS)
        return ladder, picked

    ladder_first, window_blocks = lax.map(per_row, rows)
    pair_energy = (occ_energy[:, None] + occ_energy[None, :]).reshape(OCC_PAIRS)
    window_energy = vir_energy[window_rows]
    denominator = window_energy[:, None, None] + vir_energy[None, None, :] - pair_energy[None, :, None]
    first_update = ((driver_term + ladder_first) / denominator).astype(jnp.bfloat16)
    old_rows = jnp.transpose(amplitudes[window_rows], (0, 2, 1)).astype(jnp.float32)
    delta = (first_update.astype(jnp.float32) - old_rows).astype(jnp.bfloat16)
    correction = jnp.einsum("awbd,wid->aib", window_blocks.astype(jnp.float32), delta.astype(jnp.float32))
    ladder_second = ladder_first + correction
    second_update = ((driver_term + ladder_second) / denominator).astype(jnp.bfloat16)
    return first_update, second_update
```

```python
import jax
import jax.numpy as jnp
from jax import lax
from jax.sharding import Mesh, PartitionSpec as P

OUT = ("x", "yl")
CON = ("z", "yh", "core")
CHIPS = ("x", "yl", "z", "yh")
FINE = (4, 2, 4, 2, 2)


def copy_for_each(value, axis):
    size = lax.axis_size(axis)
    return lax.all_to_all(
        jnp.broadcast_to(value[None], (size, *value.shape)), axis, 0, 0, tiled=True
    )


def swap_cores(value):
    return lax.ppermute(value, "core", [(0, 1), (1, 0)])


def on_device(fitted_factors, amplitudes, driver_term, occ_energy, vir_energy, window_rows):
    block_b, block_d, aux = fitted_factors.shape
    virtuals, _, pairs = amplitudes.shape
    window = window_rows.shape[0]
    out_index = lax.axis_index(OUT)
    con_index = lax.axis_index(CON)
    core = lax.axis_index("core")
    outs, cons = lax.axis_size(OUT), lax.axis_size(CON)
    groups = cons // 2
    half = window * block_d // outs
    parts = block_d // half

    split = amplitudes.reshape(groups, 2, block_d, block_d, pairs)
    own_t = lax.dynamic_index_in_dim(split, core, 1, False)
    other_t = swap_cores(lax.dynamic_index_in_dim(split, 1 - core, 1, False))
    other_f = swap_cores(fitted_factors)

    local = window_rows - out_index * block_b
    owned = jnp.stack(
        [
            jnp.where(
                (local[k] >= 0) & (local[k] < block_b),
                lax.dynamic_index_in_dim(
                    fitted_factors, jnp.clip(local[k], 0, block_b - 1), 0, False
                ),
                0,
            )
            for k in range(window)
        ]
    )
    tiles = lax.all_to_all(owned.reshape(outs, half, aux), OUT, 0, 0, tiled=True)
    piece = jnp.sum(tiles.astype(jnp.float32), axis=0).astype(jnp.bfloat16)
    rows = copy_for_each(piece, CHIPS)
    rows = rows.reshape(window, parts * groups * half, aux)

    def c_order(t):
        t = t.reshape(groups, parts, half, block_d, pairs)
        return t.transpose(1, 0, 2, 3, 4).reshape(parts * groups * half, block_d, pairs)

    own_t, other_t = c_order(own_t), c_order(other_t)
    part_i = jnp.arange(parts)[:, None, None]
    group_i = jnp.arange(groups)[None, :, None]
    r_i = jnp.arange(half)[None, None, :]
    c_index = ((group_i * 2 + core) * block_d + part_i * half + r_i).reshape(-1)

    at_window = (window_rows[:, None] == c_index[None, :]).astype(jnp.bfloat16)
    vectors = jnp.einsum("mc,kcq->kmq", at_window, rows, preferred_element_type=jnp.float32)
    vectors = vectors.astype(jnp.bfloat16)
    vectors = vectors + swap_cores(vectors)
    blocks = jnp.einsum(
        "kmq,bdq->kmbd", vectors, fitted_factors, preferred_element_type=jnp.float32
    ).astype(jnp.bfloat16)
    old = jnp.stack(
        [lax.dynamic_index_in_dim(amplitudes, window_rows[m], 0, False) for m in range(window)]
    )
    own_pairs = pairs // cons
    old = old.reshape(window, block_d, cons, own_pairs).transpose(2, 0, 1, 3)
    old_all = lax.all_to_all(old, CON, 0, 0, tiled=True)
    blocks_all = copy_for_each(blocks, CON)

    ladder = []
    for k in range(window):
        total = 0.0
        for f, t in ((fitted_factors, own_t), (other_f, other_t)):
            block = jnp.einsum(
                "cq,bdq->cbd", rows[k], f, preferred_element_type=jnp.float32
            ).astype(jnp.bfloat16)
            total = total + jnp.einsum(
                "cbd,cdi->ib", block, t, preferred_element_type=jnp.float32
            )
        ladder.append(total)
    ladder = jnp.stack(ladder)

    tiles = ladder.reshape(window, cons, own_pairs, block_b).transpose(1, 0, 2, 3)
    ladder_own = jnp.sum(lax.all_to_all(tiles, CON, 0, 0, tiled=True), axis=0)

    mask = window_rows[:, None] == jnp.arange(virtuals, dtype=jnp.int32)[None, :]
    window_energy = jnp.sum(jnp.where(mask, vir_energy[None, :], 0.0), axis=1)
    local_energy = lax.dynamic_slice_in_dim(vir_energy, out_index * block_b, block_b, 0)
    pair_energy = (occ_energy[:, None] + occ_energy[None, :]).reshape(-1)
    pair_energy = lax.dynamic_slice_in_dim(pair_energy, con_index * own_pairs, own_pairs, 0)
    denom = window_energy[:, None, None] + local_energy[None, None, :] - pair_energy[None, :, None]
    driver = lax.dynamic_slice_in_dim(driver_term, con_index * own_pairs, own_pairs, 1)

    first_own = ((driver + ladder_own) / denom).astype(jnp.bfloat16)
    first_all = copy_for_each(first_own, OUT)
    first_all = first_all.transpose(1, 2, 0, 3).reshape(window, own_pairs, cons, block_d)
    delta = (
        first_all.astype(jnp.float32) - old_all.transpose(1, 3, 0, 2).astype(jnp.float32)
    ).astype(jnp.bfloat16)
    correction = jnp.einsum(
        "nkmbd,mind->kib", blocks_all, delta, preferred_element_type=jnp.float32
    )
    second_own = ((driver + (ladder_own + correction)) / denom).astype(jnp.bfloat16)
    return (first_own, second_own)


def solution(mesh):
    fine = Mesh(mesh.devices.reshape(FINE), OUT + CON)
    return jax.shard_map(
        on_device,
        mesh=fine,
        in_specs=(P(OUT, CON, None), P(None, CON, None), P(None, None, OUT), P(), P(), P()),
        out_specs=(P(None, CON, OUT), P(None, CON, OUT)),
        check_vma=False,
    )
```

```python
import jax
import jax.numpy as jnp
from jax import lax
from jax.experimental import pallas as pl
from jax.experimental.pallas import tpu as pltpu
from jax.sharding import Mesh, PartitionSpec as P


OUT = ("x", "yl")
CON = ("z", "yh", "core")
CHIPS = ("x", "yl", "z", "yh")
FINE = (4, 2, 4, 2, 2)
D_STEP = 8
f32, bf16 = jnp.float32, jnp.bfloat16


def copy_for_each(value, axis):
    size = lax.axis_size(axis)
    return lax.all_to_all(
        jnp.broadcast_to(value[None], (size, *value.shape)), axis, 0, 0, tiled=True
    )


def swap_cores(value):
    return lax.ppermute(value, "core", [(0, 1), (1, 0)])


def dot_t(a, b):
    return lax.dot_general(a, b, (((1,), (1,)), ((), ())), preferred_element_type=f32)


def select_rows(local, factors):
    window = local.shape[0]
    block_b, block_d, aux = factors.shape

    def body(local_ref, f_ref, o_ref):
        row = local_ref[pl.program_id(0)]
        mine = (row >= 0) & (row < block_b)
        o_ref[...] = jnp.where(mine, f_ref[...], jnp.zeros_like(f_ref))

    def row_map(k, local_ref):
        return (jnp.clip(local_ref[k], 0, block_b - 1), 0, 0)

    return pl.pallas_call(
        body,
        grid_spec=pltpu.PrefetchScalarGridSpec(
            num_scalar_prefetch=1,
            grid=(window,),
            in_specs=[pl.BlockSpec((1, block_d, aux), row_map)],
            out_specs=pl.BlockSpec((1, block_d, aux), lambda k, _: (k, 0, 0)),
        ),
        out_shape=jax.ShapeDtypeStruct((window, block_d, aux), bf16),
        name="select_rows",
    )(local, factors)


def window_dots(vectors, factors):
    n, aux = vectors.shape
    block_d, block_b, _ = factors.shape

    def body(v_ref, f_ref, o_ref):
        o_ref[...] = dot_t(v_ref[...], f_ref[...].reshape(-1, aux)).astype(bf16)

    return pl.pallas_call(
        body,
        grid=(block_d // D_STEP,),
        in_specs=[
            pl.BlockSpec((n, aux), lambda i: (0, 0)),
            pl.BlockSpec((D_STEP, block_b, aux), lambda i: (i, 0, 0)),
        ],
        out_specs=pl.BlockSpec((n, D_STEP * block_b), lambda i: (0, i)),
        out_shape=jax.ShapeDtypeStruct((n, block_d * block_b), bf16),
        name="window_dots",
    )(vectors, factors)


def ladder_sums(core, rows, f_own, f_other, t_all, t_other, window):
    count, aux = rows.shape
    block_d, block_b, _ = f_own.shape
    _, _, c_half, pairs = t_all.shape
    steps = block_d // D_STEP

    def body(core_ref, a_ref, f1_ref, f2_ref, t1_ref, t2_ref, o_ref, lhs_ref, acc_ref):
        i = pl.program_id(0)

        @pl.when(i == 0)
        def _():
            acc_ref[...] = jnp.zeros_like(acc_ref)

        def step(f, t):
            for k in range(window):
                p = dot_t(f, a_ref[k * c_half : (k + 1) * c_half, :]).astype(bf16)
                for d in range(D_STEP):
                    lhs_ref[k * block_b : (k + 1) * block_b, d * c_half : (d + 1) * c_half] = p[
                        d * block_b : (d + 1) * block_b, :
                    ]
            acc_ref[...] += jnp.dot(lhs_ref[...], t, preferred_element_type=f32)

        @pl.when(i < steps)
        def _():
            step(f1_ref[...].reshape(-1, aux), t1_ref[...].reshape(-1, pairs))

        @pl.when(i >= steps)
        def _():
            step(f2_ref[...].reshape(-1, aux), t2_ref[...].reshape(-1, pairs))

        @pl.when(i == 2 * steps - 1)
        def _():
            o_ref[...] = acc_ref[...].T

    def first(i):
        return jnp.minimum(i, steps - 1)

    def second(i):
        return jnp.maximum(i - steps, 0)

    flops = 2 * 2 * block_d * block_b * count * (aux + pairs)
    return pl.pallas_call(
        body,
        grid_spec=pltpu.PrefetchScalarGridSpec(
            num_scalar_prefetch=1,
            grid=(2 * steps,),
            in_specs=[
                pl.BlockSpec((count, aux), lambda i, c: (0, 0)),
                pl.BlockSpec((D_STEP, block_b, aux), lambda i, c: (first(i), 0, 0)),
                pl.BlockSpec((D_STEP, block_b, aux), lambda i, c: (second(i), 0, 0)),
                pl.BlockSpec((1, D_STEP, c_half, pairs), lambda i, c: (c[0], first(i), 0, 0)),
                pl.BlockSpec((D_STEP, c_half, pairs), lambda i, c: (second(i), 0, 0)),
            ],
            out_specs=pl.BlockSpec((pairs, window * block_b), lambda i, c: (0, 0)),
            scratch_shapes=[
                pltpu.VMEM((window * block_b, D_STEP * c_half), bf16),
                pltpu.VMEM((window * block_b, pairs), f32),
            ],
        ),
        out_shape=jax.ShapeDtypeStruct((pairs, window * block_b), f32),
        cost_estimate=pl.CostEstimate(flops=flops, bytes_accessed=24_000_000, transcendentals=0),
        name="ladder_sums",
    )(core, rows, f_own, f_other, t_all, t_other)


def first_step(tiles, driver, denom, window):
    _, own_pairs, width = tiles.shape
    block_b = width // window

    def body(t_ref, d_ref, e_ref, l_ref, w_ref, o_ref):
        ladder = jnp.sum(t_ref[...], axis=0)
        l_ref[...] = ladder
        value = ((d_ref[...] + ladder) / e_ref[...]).astype(bf16)
        w_ref[...] = value
        for k in range(window):
            o_ref[k] = value[:, k * block_b : (k + 1) * block_b]

    return pl.pallas_call(
        body,
        out_shape=(
            jax.ShapeDtypeStruct((own_pairs, width), f32),
            jax.ShapeDtypeStruct((own_pairs, width), bf16),
            jax.ShapeDtypeStruct((window, own_pairs, block_b), bf16),
        ),
        name="first_step",
    )(tiles, driver, denom)


def second_step(first_all, old, blocks, ladder, driver, denom, window):
    outs, own_pairs, width = first_all.shape
    cons = blocks.shape[0]
    block_b = width // window
    per = cons // outs
    block_d = block_b // per

    def body(f_ref, p_ref, w_ref, l_ref, d_ref, e_ref, o_ref, s_ref):
        total = l_ref[...]
        for o in range(outs):
            delta = (f_ref[o].astype(f32) - p_ref[o].astype(f32)).astype(bf16)
            for m in range(window):
                for h in range(per):
                    at = m * block_b + h * block_d
                    s_ref[at : at + block_d, :] = w_ref[
                        per * o + h, m * block_d : (m + 1) * block_d, :
                    ]
            total = total + jnp.dot(delta, s_ref[...], preferred_element_type=f32)
        value = ((d_ref[...] + total) / e_ref[...]).astype(bf16)
        for k in range(window):
            o_ref[k] = value[:, k * block_b : (k + 1) * block_b]

    return pl.pallas_call(
        body,
        out_shape=jax.ShapeDtypeStruct((window, own_pairs, block_b), bf16),
        scratch_shapes=[pltpu.VMEM((width, width), bf16)],
        name="second_step",
    )(first_all, old, blocks, ladder, driver, denom)


def update(fitted_factors, amplitudes, driver_term, occ_energy, vir_energy, window_rows):
    block_b, block_d, aux = fitted_factors.shape
    virtuals, _, pairs = amplitudes.shape
    window = window_rows.shape[0]
    out_index = lax.axis_index(OUT)
    con_index = lax.axis_index(CON)
    core = lax.axis_index("core").astype(jnp.int32)
    outs, cons = lax.axis_size(OUT), lax.axis_size(CON)
    groups = cons // 2
    half = window * block_d // outs
    parts = block_d // half
    c_half = parts * groups * half
    own_pairs = pairs // cons

    owned = select_rows(window_rows - out_index.astype(jnp.int32) * block_b, fitted_factors)
    tiles = lax.all_to_all(owned.reshape(outs, half, aux), OUT, 0, 0, tiled=True)
    piece = jnp.sum(tiles.astype(f32), axis=0).astype(bf16)
    piece, factors = lax.optimization_barrier((piece, fitted_factors))
    piece, amplitudes = lax.optimization_barrier((piece, amplitudes))
    rows = copy_for_each(piece, CHIPS)
    rows = rows.reshape(window * c_half, aux)

    f_own = factors.transpose(1, 0, 2)
    f_other = swap_cores(f_own)
    t_all = amplitudes.reshape(groups, 2, parts, half, block_d, pairs)
    t_all = t_all.transpose(1, 4, 2, 0, 3, 5).reshape(2, block_d, c_half, pairs)
    t_other = swap_cores(lax.dynamic_index_in_dim(t_all, 1 - core, 0, False))

    part_i = jnp.arange(parts)[:, None, None]
    group_i = jnp.arange(groups)[None, :, None]
    r_i = jnp.arange(half)[None, None, :]
    c_index = ((group_i * 2 + core) * block_d + part_i * half + r_i).reshape(-1)

    old = jnp.concatenate(
        [lax.dynamic_slice_in_dim(amplitudes, window_rows[m], 1, 0) for m in range(window)]
    )
    width = window * block_b
    old = old.reshape(window, block_d, cons, own_pairs).transpose(2, 3, 0, 1)
    old = old.reshape(cons, -1, width)

    mask = window_rows[:, None] == jnp.arange(virtuals, dtype=jnp.int32)[None, :]
    window_energy = jnp.sum(jnp.where(mask, vir_energy[None, :], 0.0), axis=1)
    local_energy = lax.dynamic_slice_in_dim(vir_energy, out_index * block_b, block_b, 0)
    pair_energy = (occ_energy[:, None] + occ_energy[None, :]).reshape(-1)
    pair_energy = lax.dynamic_slice_in_dim(pair_energy, con_index * own_pairs, own_pairs, 0)
    denom = (window_energy[:, None] + local_energy[None, :]).reshape(1, -1) - pair_energy[:, None]
    driver = lax.dynamic_slice_in_dim(driver_term, con_index * own_pairs, own_pairs, 1)
    driver = driver.transpose(1, 0, 2).reshape(own_pairs, width)

    rows, f_own, f_other, t_all, t_other, old, denom, driver = lax.optimization_barrier(
        (rows, f_own, f_other, t_all, t_other, old, denom, driver)
    )

    at_window = (window_rows[:, None] == c_index[None, :]).astype(bf16)
    vectors = jnp.einsum(
        "mc,kcq->mkq", at_window, rows.reshape(window, c_half, aux), preferred_element_type=f32
    ).astype(bf16)
    vectors = vectors.reshape(window * window, aux)
    vectors = vectors + swap_cores(vectors)
    blocks = window_dots(vectors, f_own)
    blocks = blocks.reshape(window, window, block_d, block_b).transpose(0, 2, 1, 3)
    blocks = blocks.reshape(window * block_d, width)
    sent = jnp.concatenate(
        [jnp.broadcast_to(blocks[None], (cons, *blocks.shape)), old], axis=1
    )
    sent, rows = lax.optimization_barrier((sent, rows))
    got = lax.all_to_all(sent, CON, 0, 0, tiled=True)

    ladder = ladder_sums(core[None], rows, f_own, f_other, t_all, t_other, window)
    ladder, got = lax.optimization_barrier((ladder, got))
    tiles = lax.all_to_all(ladder.reshape(cons, own_pairs, width), CON, 0, 0, tiled=True)
    ladder_own, first_wide, first_own = first_step(tiles, driver, denom, window)
    first_all = copy_for_each(first_wide, OUT)

    old_all = got[:, window * block_d :].reshape(outs, cons // outs, own_pairs, window, block_d)
    old_all = old_all.transpose(0, 2, 3, 1, 4).reshape(outs, own_pairs, width)
    second_own = second_step(first_all, old_all, got, ladder_own, driver, denom, window)
    return (first_own, second_own)


def solution(mesh):
    fine = Mesh(mesh.devices.reshape(FINE), OUT + CON)
    return jax.shard_map(
        update,
        mesh=fine,
        in_specs=(P(OUT, CON, None), P(None, CON, None), P(None, None, OUT), P(), P(), P()),
        out_specs=(P(None, CON, OUT), P(None, CON, OUT)),
        check_vma=False,
    )
```

```python
import jax
import jax.numpy as jnp
from jax import lax
from jax.experimental import pallas as pl
from jax.experimental.pallas import tpu as pltpu
from jax.sharding import Mesh, PartitionSpec as P


OUT = ("x", "yl")
CON = ("z", "yh", "core")
CHIPS = ("x", "yl", "z", "yh")
FINE = (4, 2, 4, 2, 2)
D_STEP = 8
f32, bf16 = jnp.float32, jnp.bfloat16


def copy_for_each(value, axis):
    size = lax.axis_size(axis)
    return lax.all_to_all(
        jnp.broadcast_to(value[None], (size, *value.shape)), axis, 0, 0, tiled=True
    )


def swap_cores(value):
    return lax.ppermute(value, "core", [(0, 1), (1, 0)])


def dot_t(a, b):
    return lax.dot_general(a, b, (((1,), (1,)), ((), ())), preferred_element_type=f32)


def select_rows(local, factors):
    window = local.shape[0]
    block_b, block_d, aux = factors.shape

    def body(local_ref, f_ref, o_ref):
        row = local_ref[pl.program_id(0)]
        mine = (row >= 0) & (row < block_b)
        o_ref[...] = jnp.where(mine, f_ref[...], jnp.zeros_like(f_ref))

    def row_map(k, local_ref):
        return (jnp.clip(local_ref[k], 0, block_b - 1), 0, 0)

    return pl.pallas_call(
        body,
        grid_spec=pltpu.PrefetchScalarGridSpec(
            num_scalar_prefetch=1,
            grid=(window,),
            in_specs=[pl.BlockSpec((1, block_d, aux), row_map)],
            out_specs=pl.BlockSpec((1, block_d, aux), lambda k, _: (k, 0, 0)),
        ),
        out_shape=jax.ShapeDtypeStruct((window, block_d, aux), bf16),
        name="select_rows",
    )(local, factors)


def window_blocks(vectors, more, factors, old):
    n, aux = vectors.shape
    block_d, block_b, _ = factors.shape
    cons, tail, width = old.shape
    window = width // block_b
    steps = block_d // D_STEP
    count = window * block_d

    def body(v_ref, u_ref, f_ref, p_ref, o_ref, w_ref):
        v = v_ref[...] + u_ref[...]
        v = jnp.concatenate([v, jnp.zeros((128 - n, aux), v.dtype)])
        x = dot_t(f_ref[...].reshape(-1, aux), v).T[:n]
        i = pl.program_id(0)
        for s in range(steps):

            @pl.when(i == s)
            def _():
                for d in range(D_STEP):
                    y = x[:, d * block_b : (d + 1) * block_b]
                    for h in range(width // 128):
                        w_ref[pl.ds(h * count + s * D_STEP + d, window, stride=block_d), :] = (
                            jnp.concatenate(
                                [
                                    y[k * window : (k + 1) * window]
                                    for k in range(h * 128 // block_b, (h + 1) * 128 // block_b)
                                ],
                                axis=1,
                            )
                        )

        @pl.when(i == steps - 1)
        def _():
            for h in range(width // 128):
                w = w_ref[h * count : (h + 1) * count].astype(bf16)
                for j in range(cons):
                    o_ref[j, :count, h * 128 : (h + 1) * 128] = w
            o_ref[:, count:] = p_ref[...]

    return pl.pallas_call(
        body,
        grid=(steps,),
        in_specs=[
            pl.BlockSpec((n, aux), lambda i: (0, 0)),
            pl.BlockSpec((n, aux), lambda i: (0, 0)),
            pl.BlockSpec((D_STEP, block_b, aux), lambda i: (i, 0, 0)),
            pl.BlockSpec(old.shape, lambda i: (0, 0, 0)),
        ],
        out_specs=pl.BlockSpec((cons, count + tail, width), lambda i: (0, 0, 0)),
        out_shape=jax.ShapeDtypeStruct((cons, count + tail, width), bf16),
        scratch_shapes=[pltpu.VMEM((width // 128 * count, 128), f32)],
        name="window_blocks",
    )(vectors, more, factors, old)


def ladder_sums(core, rows, f_own, f_other, t_all, t_other, window):
    count, aux = rows.shape
    block_d, block_b, _ = f_own.shape
    _, _, c_half, pairs = t_all.shape
    steps = block_d // D_STEP

    def body(core_ref, a_ref, f1_ref, f2_ref, t1_ref, t2_ref, o_ref, lhs_ref, acc_ref):
        i = pl.program_id(0)

        @pl.when(i == 0)
        def _():
            acc_ref[...] = jnp.zeros_like(acc_ref)

        def step(f, t):
            for k in range(window):
                p = dot_t(f, a_ref[k * c_half : (k + 1) * c_half, :]).astype(bf16)
                for d in range(D_STEP):
                    lhs_ref[k * block_b : (k + 1) * block_b, d * c_half : (d + 1) * c_half] = p[
                        d * block_b : (d + 1) * block_b, :
                    ]
            acc_ref[...] += jnp.dot(lhs_ref[...], t, preferred_element_type=f32)

        @pl.when(i < steps)
        def _():
            step(f1_ref[...].reshape(-1, aux), t1_ref[...].reshape(-1, pairs))

        @pl.when(i >= steps)
        def _():
            step(f2_ref[...].reshape(-1, aux), t2_ref[...].reshape(-1, pairs))

        @pl.when(i == 2 * steps - 1)
        def _():
            o_ref[...] = acc_ref[...].T

    def first(i):
        return jnp.minimum(i, steps - 1)

    def second(i):
        return jnp.maximum(i - steps, 0)

    flops = 2 * 2 * block_d * block_b * count * (aux + pairs)
    return pl.pallas_call(
        body,
        grid_spec=pltpu.PrefetchScalarGridSpec(
            num_scalar_prefetch=1,
            grid=(2 * steps,),
            in_specs=[
                pl.BlockSpec((count, aux), lambda i, c: (0, 0)),
                pl.BlockSpec((D_STEP, block_b, aux), lambda i, c: (first(i), 0, 0)),
                pl.BlockSpec((D_STEP, block_b, aux), lambda i, c: (second(i), 0, 0)),
                pl.BlockSpec((1, D_STEP, c_half, pairs), lambda i, c: (c[0], first(i), 0, 0)),
                pl.BlockSpec((D_STEP, c_half, pairs), lambda i, c: (second(i), 0, 0)),
            ],
            out_specs=pl.BlockSpec((pairs, window * block_b), lambda i, c: (0, 0)),
            scratch_shapes=[
                pltpu.VMEM((window * block_b, D_STEP * c_half), bf16),
                pltpu.VMEM((window * block_b, pairs), f32),
            ],
        ),
        out_shape=jax.ShapeDtypeStruct((pairs, window * block_b), f32),
        cost_estimate=pl.CostEstimate(flops=flops, bytes_accessed=24_000_000, transcendentals=0),
        name="ladder_sums",
    )(core, rows, f_own, f_other, t_all, t_other)


def first_step(tiles, driver, denom, window, outs):
    _, own_pairs, width = tiles.shape
    block_b = width // window

    def body(t_ref, d_ref, e_ref, l_ref, w_ref, o_ref):
        ladder = jnp.sum(t_ref[...], axis=0)
        l_ref[...] = ladder
        value = ((d_ref[...] + ladder) / e_ref[...]).astype(bf16)
        for o in range(outs):
            w_ref[o] = value
        for k in range(window):
            o_ref[k] = value[:, k * block_b : (k + 1) * block_b]

    return pl.pallas_call(
        body,
        out_shape=(
            jax.ShapeDtypeStruct((own_pairs, width), f32),
            jax.ShapeDtypeStruct((outs, own_pairs, width), bf16),
            jax.ShapeDtypeStruct((window, own_pairs, block_b), bf16),
        ),
        name="first_step",
    )(tiles, driver, denom)


def second_step(first_all, old, blocks, ladder, driver, denom, window):
    outs, own_pairs, width = first_all.shape
    cons = blocks.shape[0]
    block_b = width // window
    per = cons // outs
    block_d = block_b // per

    def body(f_ref, p_ref, w_ref, l_ref, d_ref, e_ref, o_ref, s_ref):
        total = l_ref[...]
        for o in range(outs):
            delta = (f_ref[o].astype(f32) - p_ref[o].astype(f32)).astype(bf16)
            for m in range(window):
                for h in range(per):
                    at = m * block_b + h * block_d
                    s_ref[at : at + block_d, :] = w_ref[
                        per * o + h, m * block_d : (m + 1) * block_d, :
                    ]
            total = total + jnp.dot(delta, s_ref[...], preferred_element_type=f32)
        value = ((d_ref[...] + total) / e_ref[...]).astype(bf16)
        for k in range(window):
            o_ref[k] = value[:, k * block_b : (k + 1) * block_b]

    return pl.pallas_call(
        body,
        out_shape=jax.ShapeDtypeStruct((window, own_pairs, block_b), bf16),
        scratch_shapes=[pltpu.VMEM((width, width), bf16)],
        name="second_step",
    )(first_all, old, blocks, ladder, driver, denom)


def update(fitted_factors, amplitudes, driver_term, occ_energy, vir_energy, window_rows):
    block_b, block_d, aux = fitted_factors.shape
    virtuals, _, pairs = amplitudes.shape
    window = window_rows.shape[0]
    out_index = lax.axis_index(OUT)
    con_index = lax.axis_index(CON)
    core = lax.axis_index("core").astype(jnp.int32)
    outs, cons = lax.axis_size(OUT), lax.axis_size(CON)
    groups = cons // 2
    half = window * block_d // outs
    parts = block_d // half
    c_half = parts * groups * half
    own_pairs = pairs // cons

    owned = select_rows(window_rows - out_index.astype(jnp.int32) * block_b, fitted_factors)
    tiles = lax.all_to_all(owned.reshape(outs, half, aux), OUT, 0, 0, tiled=True)
    piece = jnp.sum(tiles.astype(f32), axis=0).astype(bf16)
    piece, factors = lax.optimization_barrier((piece, fitted_factors))
    piece, amplitudes = lax.optimization_barrier((piece, amplitudes))
    rows = copy_for_each(piece, CHIPS)
    rows = rows.reshape(window * c_half, aux)

    f_own = factors.transpose(1, 0, 2)
    f_other = swap_cores(f_own)
    t_all = amplitudes.reshape(groups, 2, parts, half, block_d, pairs)
    t_all = t_all.transpose(1, 4, 2, 0, 3, 5).reshape(2, block_d, c_half, pairs)
    t_other = swap_cores(lax.dynamic_index_in_dim(t_all, 1 - core, 0, False))

    part_i = jnp.arange(parts)[:, None, None]
    group_i = jnp.arange(groups)[None, :, None]
    r_i = jnp.arange(half)[None, None, :]
    c_index = ((group_i * 2 + core) * block_d + part_i * half + r_i).reshape(-1)

    old = jnp.concatenate(
        [lax.dynamic_slice_in_dim(amplitudes, window_rows[m], 1, 0) for m in range(window)]
    )
    width = window * block_b
    old = old.reshape(window, block_d, cons, own_pairs).transpose(2, 3, 0, 1)
    old = old.reshape(cons, -1, width)

    mask = window_rows[:, None] == jnp.arange(virtuals, dtype=jnp.int32)[None, :]
    window_energy = jnp.sum(jnp.where(mask, vir_energy[None, :], 0.0), axis=1)
    local_energy = lax.dynamic_slice_in_dim(vir_energy, out_index * block_b, block_b, 0)
    pair_energy = (occ_energy[:, None] + occ_energy[None, :]).reshape(-1)
    pair_energy = lax.dynamic_slice_in_dim(pair_energy, con_index * own_pairs, own_pairs, 0)
    denom = (window_energy[:, None] + local_energy[None, :]).reshape(1, -1) - pair_energy[:, None]
    driver = lax.dynamic_slice_in_dim(driver_term, con_index * own_pairs, own_pairs, 1)
    driver = driver.transpose(1, 0, 2).reshape(own_pairs, width)

    rows, f_own, f_other, t_all, t_other, old, denom, driver = lax.optimization_barrier(
        (rows, f_own, f_other, t_all, t_other, old, denom, driver)
    )

    at_window = (window_rows[:, None] == c_index[None, :]).astype(bf16)
    vectors = jnp.einsum(
        "mc,kcq->kmq", at_window, rows.reshape(window, c_half, aux), preferred_element_type=f32
    ).astype(bf16)
    vectors = vectors.reshape(window * window, aux)
    sent = window_blocks(vectors, swap_cores(vectors), f_own, old)
    sent, rows = lax.optimization_barrier((sent, rows))
    got = lax.all_to_all(sent, CON, 0, 0, tiled=True)

    ladder = ladder_sums(core[None], rows, f_own, f_other, t_all, t_other, window)
    ladder, got = lax.optimization_barrier((ladder, got))
    tiles = lax.all_to_all(ladder.reshape(cons, own_pairs, width), CON, 0, 0, tiled=True)
    ladder_own, first_wide, first_own = first_step(tiles, driver, denom, window, outs)
    first_all = lax.all_to_all(first_wide, OUT, 0, 0, tiled=True)

    old_all = got[:, window * block_d :].reshape(outs, cons // outs, own_pairs, window, block_d)
    old_all = old_all.transpose(0, 2, 3, 1, 4).reshape(outs, own_pairs, width)
    second_own = second_step(first_all, old_all, got, ladder_own, driver, denom, window)
    return (first_own, second_own)


def solution(mesh):
    fine = Mesh(mesh.devices.reshape(FINE), OUT + CON)
    return jax.shard_map(
        update,
        mesh=fine,
        in_specs=(P(OUT, CON, None), P(None, CON, None), P(None, None, OUT), P(), P(), P()),
        out_specs=(P(None, CON, OUT), P(None, CON, OUT)),
        check_vma=False,
    )
```

```python
import jax
import jax.numpy as jnp
from jax import lax
from jax.experimental import pallas as pl
from jax.experimental.pallas import tpu as pltpu
from jax.sharding import Mesh, PartitionSpec as P


OUT = ("x", "yl")
CON = ("z", "yh", "core")
CHIPS = ("x", "yl", "z", "yh")
FINE = (4, 2, 4, 2, 2)
D_STEP = 8
f32, bf16 = jnp.float32, jnp.bfloat16


def copy_for_each(value, axis):
    size = lax.axis_size(axis)
    return lax.all_to_all(
        jnp.broadcast_to(value[None], (size, *value.shape)), axis, 0, 0, tiled=True
    )


def swap_cores(value):
    return lax.ppermute(value, "core", [(0, 1), (1, 0)])


def dot_t(a, b):
    return lax.dot_general(a, b, (((1,), (1,)), ((), ())), preferred_element_type=f32)


def select_rows(local, factors):
    window = local.shape[0]
    block_b, block_d, aux = factors.shape

    def body(local_ref, f_ref, o_ref):
        row = local_ref[pl.program_id(0)]
        mine = (row >= 0) & (row < block_b)
        o_ref[...] = jnp.where(mine, f_ref[...], jnp.zeros_like(f_ref))

    def row_map(k, local_ref):
        return (jnp.clip(local_ref[k], 0, block_b - 1), 0, 0)

    return pl.pallas_call(
        body,
        grid_spec=pltpu.PrefetchScalarGridSpec(
            num_scalar_prefetch=1,
            grid=(window,),
            in_specs=[pl.BlockSpec((1, block_d, aux), row_map)],
            out_specs=pl.BlockSpec((1, block_d, aux), lambda k, _: (k, 0, 0)),
        ),
        out_shape=jax.ShapeDtypeStruct((window, block_d, aux), bf16),
        name="select_rows",
    )(local, factors)


def window_blocks(vectors, more, factors, old):
    n, aux = vectors.shape
    block_d, block_b, _ = factors.shape
    cons, own_pairs, count = old.shape
    window = count // block_d
    width = window * block_b
    tail = own_pairs * count // width
    steps = block_d // D_STEP

    def body(v_ref, u_ref, f_ref, p_ref, o_ref, w_ref):
        v = v_ref[...] + u_ref[...]
        v = jnp.concatenate([v, jnp.zeros((128 - n, aux), v.dtype)])
        x = dot_t(f_ref[...].reshape(-1, aux), v).T[:n]
        i = pl.program_id(0)
        for s in range(steps):

            @pl.when(i == s)
            def _():
                for d in range(D_STEP):
                    y = x[:, d * block_b : (d + 1) * block_b]
                    for h in range(width // 128):
                        w_ref[pl.ds(h * count + s * D_STEP + d, window, stride=block_d), :] = (
                            jnp.concatenate(
                                [
                                    y[k * window : (k + 1) * window]
                                    for k in range(h * 128 // block_b, (h + 1) * 128 // block_b)
                                ],
                                axis=1,
                            )
                        )

        @pl.when(i == steps - 1)
        def _():
            for h in range(width // 128):
                w = w_ref[h * count : (h + 1) * count].astype(bf16)
                for j in range(cons):
                    o_ref[j, :count, h * 128 : (h + 1) * 128] = w
            for j in range(width // count):
                o_ref[:, count:, j * count : (j + 1) * count] = p_ref[
                    :, j * tail : (j + 1) * tail, :
                ]

    return pl.pallas_call(
        body,
        grid=(steps,),
        in_specs=[
            pl.BlockSpec((n, aux), lambda i: (0, 0)),
            pl.BlockSpec((n, aux), lambda i: (0, 0)),
            pl.BlockSpec((D_STEP, block_b, aux), lambda i: (i, 0, 0)),
            pl.BlockSpec(old.shape, lambda i: (0, 0, 0)),
        ],
        out_specs=pl.BlockSpec((cons, count + tail, width), lambda i: (0, 0, 0)),
        out_shape=jax.ShapeDtypeStruct((cons, count + tail, width), bf16),
        scratch_shapes=[pltpu.VMEM((width // 128 * count, 128), f32)],
        name="window_blocks",
    )(vectors, more, factors, old)


def old_rows(window_rows, amplitudes):
    window = window_rows.shape[0]
    _, block_d, pairs = amplitudes.shape

    def body(*refs):
        x = jnp.concatenate([r[0].astype(f32) for r in refs[1:-1]], axis=0)
        refs[-1][...] = x.T.astype(bf16)

    def at(m):
        return pl.BlockSpec((1, block_d, pairs), lambda i, w: (w[m], 0, 0))

    return pl.pallas_call(
        body,
        grid_spec=pltpu.PrefetchScalarGridSpec(
            num_scalar_prefetch=1,
            grid=(1,),
            in_specs=[at(m) for m in range(window)],
            out_specs=pl.BlockSpec((pairs, window * block_d), lambda i, w: (0, 0)),
        ),
        out_shape=jax.ShapeDtypeStruct((pairs, window * block_d), bf16),
        name="old_rows",
    )(window_rows, *([amplitudes] * window))


def ladder_sums(core, rows, f_own, f_other, t_all, t_other, window):
    count, aux = rows.shape
    block_d, block_b, _ = f_own.shape
    _, _, c_half, pairs = t_all.shape
    steps = block_d // D_STEP

    def body(core_ref, a_ref, f1_ref, f2_ref, t1_ref, t2_ref, o_ref, lhs_ref, acc_ref):
        i = pl.program_id(0)

        @pl.when(i == 0)
        def _():
            acc_ref[...] = jnp.zeros_like(acc_ref)

        def step(f, t):
            for k in range(window):
                p = dot_t(f, a_ref[k * c_half : (k + 1) * c_half, :]).astype(bf16)
                for d in range(D_STEP):
                    lhs_ref[k * block_b : (k + 1) * block_b, d * c_half : (d + 1) * c_half] = p[
                        d * block_b : (d + 1) * block_b, :
                    ]
            acc_ref[...] += jnp.dot(lhs_ref[...], t, preferred_element_type=f32)

        @pl.when(i < steps)
        def _():
            step(f1_ref[...].reshape(-1, aux), t1_ref[...].reshape(-1, pairs))

        @pl.when(i >= steps)
        def _():
            step(f2_ref[...].reshape(-1, aux), t2_ref[...].reshape(-1, pairs))

        @pl.when(i == 2 * steps - 1)
        def _():
            o_ref[...] = acc_ref[...].T

    def first(i):
        return jnp.minimum(i, steps - 1)

    def second(i):
        return jnp.maximum(i - steps, 0)

    flops = 2 * 2 * block_d * block_b * count * (aux + pairs)
    return pl.pallas_call(
        body,
        grid_spec=pltpu.PrefetchScalarGridSpec(
            num_scalar_prefetch=1,
            grid=(2 * steps,),
            in_specs=[
                pl.BlockSpec((count, aux), lambda i, c: (0, 0)),
                pl.BlockSpec((D_STEP, block_b, aux), lambda i, c: (first(i), 0, 0)),
                pl.BlockSpec((D_STEP, block_b, aux), lambda i, c: (second(i), 0, 0)),
                pl.BlockSpec((1, D_STEP, c_half, pairs), lambda i, c: (c[0], first(i), 0, 0)),
                pl.BlockSpec((1, D_STEP, c_half, pairs), lambda i, c: (c[0], second(i), 0, 0)),
            ],
            out_specs=pl.BlockSpec((pairs, window * block_b), lambda i, c: (0, 0)),
            scratch_shapes=[
                pltpu.VMEM((window * block_b, D_STEP * c_half), bf16),
                pltpu.VMEM((window * block_b, pairs), f32),
            ],
        ),
        out_shape=jax.ShapeDtypeStruct((pairs, window * block_b), f32),
        cost_estimate=pl.CostEstimate(flops=flops, bytes_accessed=24_000_000, transcendentals=0),
        name="ladder_sums",
    )(core, rows, f_own, f_other, t_all, t_other)


def first_step(tiles, driver, denom, window, outs):
    _, own_pairs, width = tiles.shape
    block_b = width // window

    def body(t_ref, d_ref, e_ref, l_ref, w_ref, o_ref):
        ladder = jnp.sum(t_ref[...], axis=0)
        l_ref[...] = ladder
        value = ((d_ref[...] + ladder) / e_ref[...]).astype(bf16)
        for o in range(outs):
            w_ref[o] = value
        for k in range(window):
            o_ref[k] = value[:, k * block_b : (k + 1) * block_b]

    return pl.pallas_call(
        body,
        out_shape=(
            jax.ShapeDtypeStruct((own_pairs, width), f32),
            jax.ShapeDtypeStruct((outs, own_pairs, width), bf16),
            jax.ShapeDtypeStruct((window, own_pairs, block_b), bf16),
        ),
        name="first_step",
    )(tiles, driver, denom)


def second_step(first_all, blocks, ladder, driver, denom, window):
    outs, own_pairs, width = first_all.shape
    cons = blocks.shape[0]
    block_b = width // window
    per = cons // outs
    block_d = block_b // per

    def body(f_ref, w_ref, l_ref, d_ref, e_ref, o_ref, s_ref):
        total = l_ref[...]
        count = window * block_d
        for o in range(outs):
            tails = [w_ref[per * o + h, count:, :].astype(f32) for h in range(per)]
            old = [
                jnp.concatenate(
                    [t[:, j * count : (j + 1) * count] for j in range(width // count)], axis=0
                )
                for t in tails
            ]
            old = jnp.concatenate(
                [
                    old[h][:, m * block_d : (m + 1) * block_d]
                    for m in range(window)
                    for h in range(per)
                ],
                axis=1,
            )
            delta = (f_ref[o].astype(f32) - old).astype(bf16)
            for m in range(window):
                for h in range(per):
                    at = m * block_b + h * block_d
                    s_ref[at : at + block_d, :] = w_ref[
                        per * o + h, m * block_d : (m + 1) * block_d, :
                    ]
            total = total + jnp.dot(delta, s_ref[...], preferred_element_type=f32)
        value = ((d_ref[...] + total) / e_ref[...]).astype(bf16)
        for k in range(window):
            o_ref[k] = value[:, k * block_b : (k + 1) * block_b]

    return pl.pallas_call(
        body,
        out_shape=jax.ShapeDtypeStruct((window, own_pairs, block_b), bf16),
        scratch_shapes=[pltpu.VMEM((width, width), bf16)],
        name="second_step",
    )(first_all, blocks, ladder, driver, denom)


def update(fitted_factors, amplitudes, driver_term, occ_energy, vir_energy, window_rows):
    block_b, block_d, aux = fitted_factors.shape
    virtuals, _, pairs = amplitudes.shape
    window = window_rows.shape[0]
    out_index = lax.axis_index(OUT)
    con_index = lax.axis_index(CON)
    core = lax.axis_index("core").astype(jnp.int32)
    outs, cons = lax.axis_size(OUT), lax.axis_size(CON)
    groups = cons // 2
    half = window * block_d // outs
    parts = block_d // half
    c_half = parts * groups * half
    own_pairs = pairs // cons

    owned = select_rows(window_rows - out_index.astype(jnp.int32) * block_b, fitted_factors)
    tiles = lax.all_to_all(owned.reshape(outs, half, aux), OUT, 0, 0, tiled=True)
    piece = jnp.sum(tiles.astype(f32), axis=0).astype(bf16)
    piece, factors = lax.optimization_barrier((piece, fitted_factors))
    piece, amplitudes = lax.optimization_barrier((piece, amplitudes))
    rows = copy_for_each(piece, CHIPS)
    rows = rows.reshape(window * c_half, aux)

    f_own = factors.transpose(1, 0, 2)
    f_other = swap_cores(f_own)
    t_all = amplitudes.reshape(groups, 2, parts, half, block_d, pairs)
    t_all = t_all.transpose(1, 4, 2, 0, 3, 5).reshape(2, block_d, c_half, pairs)
    t_other = swap_cores(t_all)

    part_i = jnp.arange(parts)[:, None, None]
    group_i = jnp.arange(groups)[None, :, None]
    r_i = jnp.arange(half)[None, None, :]
    c_index = ((group_i * 2 + core) * block_d + part_i * half + r_i).reshape(-1)

    width = window * block_b
    old = old_rows(window_rows, amplitudes).reshape(cons, own_pairs, window * block_d)

    rows, f_own, t_all, old = lax.optimization_barrier((rows, f_own, t_all, old))

    at_window = (window_rows[:, None] == c_index[None, :]).astype(bf16)
    vectors = jnp.einsum(
        "mc,kcq->kmq", at_window, rows.reshape(window, c_half, aux), preferred_element_type=f32
    ).astype(bf16)
    vectors = vectors.reshape(window * window, aux)
    sent = window_blocks(vectors, swap_cores(vectors), f_own, old)
    sent, rows = lax.optimization_barrier((sent, rows))
    got = lax.all_to_all(sent, CON, 0, 0, tiled=True)

    ladder = ladder_sums(core[None], rows, f_own, f_other, t_all, t_other, window)
    ladder, got, driver_term, occ_energy, vir_energy = lax.optimization_barrier(
        (ladder, got, driver_term, occ_energy, vir_energy)
    )
    tiles = lax.all_to_all(ladder.reshape(cons, own_pairs, width), CON, 0, 0, tiled=True)

    mask = window_rows[:, None] == jnp.arange(virtuals, dtype=jnp.int32)[None, :]
    window_energy = jnp.sum(jnp.where(mask, vir_energy[None, :], 0.0), axis=1)
    local_energy = lax.dynamic_slice_in_dim(vir_energy, out_index * block_b, block_b, 0)
    pair_energy = (occ_energy[:, None] + occ_energy[None, :]).reshape(-1)
    pair_energy = lax.dynamic_slice_in_dim(pair_energy, con_index * own_pairs, own_pairs, 0)
    denom = (window_energy[:, None] + local_energy[None, :]).reshape(1, -1) - pair_energy[:, None]
    driver = lax.dynamic_slice_in_dim(driver_term, con_index * own_pairs, own_pairs, 1)
    driver = driver.transpose(1, 0, 2).reshape(own_pairs, width)

    ladder_own, first_wide, first_own = first_step(tiles, driver, denom, window, outs)
    first_all = lax.all_to_all(first_wide, OUT, 0, 0, tiled=True)

    second_own = second_step(first_all, got, ladder_own, driver, denom, window)
    return (first_own, second_own)


def solution(mesh):
    fine = Mesh(mesh.devices.reshape(FINE), OUT + CON)
    return jax.shard_map(
        update,
        mesh=fine,
        in_specs=(P(OUT, CON, None), P(None, CON, None), P(None, None, OUT), P(), P(), P()),
        out_specs=(P(None, CON, OUT), P(None, CON, OUT)),
        check_vma=False,
    )
```

```python
import jax
import jax.numpy as jnp
from jax import lax
from jax.experimental import pallas as pl
from jax.experimental.pallas import tpu as pltpu
from jax.sharding import Mesh, PartitionSpec as P


OUT = ("x", "yl")
CON = ("z", "yh", "core")
CHIPS = ("x", "yl", "z", "yh")
FINE = (4, 2, 4, 2, 2)
D_STEP = 8
f32, bf16 = jnp.float32, jnp.bfloat16


def copy_for_each(value, axis):
    size = lax.axis_size(axis)
    return lax.all_to_all(
        jnp.broadcast_to(value[None], (size, *value.shape)), axis, 0, 0, tiled=True
    )


def swap_cores(value):
    return lax.ppermute(value, "core", [(0, 1), (1, 0)])


def dot_t(a, b):
    return lax.dot_general(a, b, (((1,), (1,)), ((), ())), preferred_element_type=f32)


def select_rows(window_rows, out_index, factors):
    window = window_rows.shape[0]
    block_b, block_d, aux = factors.shape

    def body(w_ref, o_index, *refs):
        for k in range(window):
            row = w_ref[k] - o_index[0] * block_b
            mine = (row >= 0) & (row < block_b)
            refs[-1][k] = jnp.where(mine, refs[k][0], jnp.zeros_like(refs[k][0]))

    def at(k):
        def row_map(i, w_ref, o_index):
            return (jnp.clip(w_ref[k] - o_index[0] * block_b, 0, block_b - 1), 0, 0)

        return pl.BlockSpec((1, block_d, aux), row_map)

    return pl.pallas_call(
        body,
        grid_spec=pltpu.PrefetchScalarGridSpec(
            num_scalar_prefetch=2,
            grid=(1,),
            in_specs=[at(k) for k in range(window)],
            out_specs=pl.BlockSpec((window, block_d, aux), lambda i, w, o: (0, 0, 0)),
        ),
        out_shape=jax.ShapeDtypeStruct((window, block_d, aux), bf16),
        name="select_rows",
    )(window_rows, out_index, *([factors] * window))


def window_vectors(window_rows, core, rows, block_d):
    window = window_rows.shape[0]
    _, _, _, half, aux = rows.shape

    def body(w_ref, c_ref, *refs):
        for m in range(window):
            c = w_ref[m]
            mine = (c // block_d) % 2 == c_ref[0]
            r = lax.broadcasted_iota(jnp.int32, (half, aux), 0)
            keep = (r == c % half) & mine
            for k in range(window):
                tile = refs[m][k, 0, 0].astype(f32)
                row = jnp.sum(jnp.where(keep, tile, 0.0), axis=0, keepdims=True)
                refs[-1][k * window + m : k * window + m + 1, :] = row

    def at(m):
        def tile_map(i, w_ref, c_ref):
            c = w_ref[m]
            return (0, (c % block_d) // half, c // (2 * block_d), 0, 0)

        return pl.BlockSpec((window, 1, 1, half, aux), tile_map)

    return pl.pallas_call(
        body,
        grid_spec=pltpu.PrefetchScalarGridSpec(
            num_scalar_prefetch=2,
            grid=(1,),
            in_specs=[at(m) for m in range(window)],
            out_specs=pl.BlockSpec((window * window, aux), lambda i, w, c: (0, 0)),
        ),
        out_shape=jax.ShapeDtypeStruct((window * window, aux), f32),
        name="window_vectors",
    )(window_rows, core, *([rows] * window))


def window_blocks(vectors, more, factors, old):
    n, aux = vectors.shape
    block_d, block_b, _ = factors.shape
    chips, cores, own_pairs, count = old.shape
    window = count // block_d
    width = window * block_b
    tail = own_pairs * count // width
    steps = block_d // D_STEP

    def body(v_ref, u_ref, f_ref, p_ref, o_ref, w_ref):
        v = v_ref[...] + u_ref[...]
        v = jnp.concatenate([v, jnp.zeros((128 - n, aux), v.dtype)])
        x = dot_t(f_ref[...].reshape(-1, aux), v).T[:n]
        i = pl.program_id(0)
        for s in range(steps):

            @pl.when(i == s)
            def _():
                for d in range(D_STEP):
                    y = x[:, d * block_b : (d + 1) * block_b]
                    for h in range(width // 128):
                        w_ref[pl.ds(h * count + s * D_STEP + d, window, stride=block_d), :] = (
                            jnp.concatenate(
                                [
                                    y[k * window : (k + 1) * window]
                                    for k in range(h * 128 // block_b, (h + 1) * 128 // block_b)
                                ],
                                axis=1,
                            )
                        )

        @pl.when(i == steps - 1)
        def _():
            for h in range(width // 128):
                w = w_ref[h * count : (h + 1) * count].astype(bf16)
                for j in range(chips):
                    o_ref[j, :count, h * 128 : (h + 1) * 128] = w
            for h in range(cores):
                at = count + h * tail
                for j in range(width // count):
                    o_ref[:, at : at + tail, j * count : (j + 1) * count] = p_ref[
                        :, h, j * tail : (j + 1) * tail, :
                    ]

    return pl.pallas_call(
        body,
        grid=(steps,),
        in_specs=[
            pl.BlockSpec((n, aux), lambda i: (0, 0)),
            pl.BlockSpec((n, aux), lambda i: (0, 0)),
            pl.BlockSpec((D_STEP, block_b, aux), lambda i: (i, 0, 0)),
            pl.BlockSpec(old.shape, lambda i: (0, 0, 0, 0)),
        ],
        out_specs=pl.BlockSpec((chips, count + cores * tail, width), lambda i: (0, 0, 0)),
        out_shape=jax.ShapeDtypeStruct((chips, count + cores * tail, width), bf16),
        scratch_shapes=[pltpu.VMEM((width // 128 * count, 128), f32)],
        name="window_blocks",
    )(vectors, more, factors, old)


def old_rows(window_rows, amplitudes):
    window = window_rows.shape[0]
    _, block_d, pairs = amplitudes.shape

    def body(*refs):
        x = jnp.concatenate([r[0].astype(f32) for r in refs[1:-1]], axis=0)
        refs[-1][...] = x.T.astype(bf16)

    def at(m):
        return pl.BlockSpec((1, block_d, pairs), lambda i, w: (w[m], 0, 0))

    return pl.pallas_call(
        body,
        grid_spec=pltpu.PrefetchScalarGridSpec(
            num_scalar_prefetch=1,
            grid=(1,),
            in_specs=[at(m) for m in range(window)],
            out_specs=pl.BlockSpec((pairs, window * block_d), lambda i, w: (0, 0)),
        ),
        out_shape=jax.ShapeDtypeStruct((pairs, window * block_d), bf16),
        name="old_rows",
    )(window_rows, *([amplitudes] * window))


def ladder_sums(core, rows, f_own, f_other, t_all, t_other, window):
    count, aux = rows.shape
    block_d, block_b, _ = f_own.shape
    _, _, c_half, pairs = t_all.shape
    steps = block_d // D_STEP

    def body(core_ref, a_ref, f1_ref, f2_ref, t1_ref, t2_ref, o_ref, lhs_ref, acc_ref):
        i = pl.program_id(0)

        @pl.when(i == 0)
        def _():
            acc_ref[...] = jnp.zeros_like(acc_ref)

        def step(f, t):
            for k in range(window):
                p = dot_t(f, a_ref[k * c_half : (k + 1) * c_half, :]).astype(bf16)
                for d in range(D_STEP):
                    lhs_ref[k * block_b : (k + 1) * block_b, d * c_half : (d + 1) * c_half] = p[
                        d * block_b : (d + 1) * block_b, :
                    ]
            acc_ref[...] += jnp.dot(lhs_ref[...], t, preferred_element_type=f32)

        @pl.when(i < steps)
        def _():
            step(f1_ref[...].reshape(-1, aux), t1_ref[...].reshape(-1, pairs))

        @pl.when(i >= steps)
        def _():
            step(f2_ref[...].reshape(-1, aux), t2_ref[...].reshape(-1, pairs))

        @pl.when(i == 2 * steps - 1)
        def _():
            o_ref[...] = acc_ref[...].T

    def first(i):
        return jnp.minimum(i, steps - 1)

    def second(i):
        return jnp.maximum(i - steps, 0)

    flops = 2 * 2 * block_d * block_b * count * (aux + pairs)
    return pl.pallas_call(
        body,
        grid_spec=pltpu.PrefetchScalarGridSpec(
            num_scalar_prefetch=1,
            grid=(2 * steps,),
            in_specs=[
                pl.BlockSpec((count, aux), lambda i, c: (0, 0)),
                pl.BlockSpec((D_STEP, block_b, aux), lambda i, c: (first(i), 0, 0)),
                pl.BlockSpec((D_STEP, block_b, aux), lambda i, c: (second(i), 0, 0)),
                pl.BlockSpec((1, D_STEP, c_half, pairs), lambda i, c: (c[0], first(i), 0, 0)),
                pl.BlockSpec((1, D_STEP, c_half, pairs), lambda i, c: (c[0], second(i), 0, 0)),
            ],
            out_specs=pl.BlockSpec((pairs, window * block_b), lambda i, c: (0, 0)),
            scratch_shapes=[
                pltpu.VMEM((window * block_b, D_STEP * c_half), bf16),
                pltpu.VMEM((window * block_b, pairs), f32),
            ],
        ),
        out_shape=jax.ShapeDtypeStruct((pairs, window * block_b), f32),
        cost_estimate=pl.CostEstimate(flops=flops, bytes_accessed=24_000_000, transcendentals=0),
        name="ladder_sums",
    )(core, rows, f_own, f_other, t_all, t_other)


def first_step(tiles, driver, denom, window, outs):
    _, own_pairs, width = tiles.shape
    block_b = width // window

    def body(t_ref, d_ref, e_ref, l_ref, w_ref, o_ref):
        ladder = jnp.sum(t_ref[...], axis=0)
        l_ref[...] = ladder
        value = ((d_ref[...] + ladder) / e_ref[...]).astype(bf16)
        for o in range(outs):
            w_ref[o] = value
        for k in range(window):
            o_ref[k] = value[:, k * block_b : (k + 1) * block_b]

    return pl.pallas_call(
        body,
        out_shape=(
            jax.ShapeDtypeStruct((own_pairs, width), f32),
            jax.ShapeDtypeStruct((outs, own_pairs, width), bf16),
            jax.ShapeDtypeStruct((window, own_pairs, block_b), bf16),
        ),
        name="first_step",
    )(tiles, driver, denom)


def second_step(core, first_all, blocks, other, ladder, driver, denom, window):
    outs, own_pairs, width = first_all.shape
    block_b = width // window
    block_d = block_b // 2
    count = window * block_d
    tail = own_pairs * count // width

    def body(c_ref, f_ref, w_ref, x_ref, l_ref, d_ref, e_ref, o_ref, s_ref):
        total = l_ref[...]
        south = c_ref[0] == 0
        for o in range(outs):
            mine, theirs = w_ref[o, :count, :], x_ref[o, :count, :]
            halves = (jnp.where(south, mine, theirs), jnp.where(south, theirs, mine))
            olds = []
            for ref in (w_ref, x_ref):
                t = jnp.where(
                    south, ref[o, count : count + tail, :], ref[o, count + tail :, :]
                ).astype(f32)
                olds.append(
                    jnp.concatenate(
                        [t[:, j * count : (j + 1) * count] for j in range(width // count)], axis=0
                    )
                )
            olds = (jnp.where(south, olds[0], olds[1]), jnp.where(south, olds[1], olds[0]))
            old = jnp.concatenate(
                [
                    olds[h][:, m * block_d : (m + 1) * block_d]
                    for m in range(window)
                    for h in range(2)
                ],
                axis=1,
            )
            delta = (f_ref[o].astype(f32) - old).astype(bf16)
            for m in range(window):
                for h in range(2):
                    at = m * block_b + h * block_d
                    s_ref[at : at + block_d, :] = halves[h][m * block_d : (m + 1) * block_d, :]
            total = total + jnp.dot(delta, s_ref[...], preferred_element_type=f32)
        value = ((d_ref[...] + total) / e_ref[...]).astype(bf16)
        for k in range(window):
            o_ref[k] = value[:, k * block_b : (k + 1) * block_b]

    whole = [first_all, blocks, other, ladder, driver, denom]
    return pl.pallas_call(
        body,
        grid_spec=pltpu.PrefetchScalarGridSpec(
            num_scalar_prefetch=1,
            grid=(1,),
            in_specs=[pl.BlockSpec(x.shape, lambda i, c, n=x.ndim: (0,) * n) for x in whole],
            out_specs=pl.BlockSpec((window, own_pairs, block_b), lambda i, c: (0, 0, 0)),
            scratch_shapes=[pltpu.VMEM((width, width), bf16)],
        ),
        out_shape=jax.ShapeDtypeStruct((window, own_pairs, block_b), bf16),
        name="second_step",
    )(core, *whole)


def update(fitted_factors, amplitudes, driver_term, occ_energy, vir_energy, window_rows):
    block_b, block_d, aux = fitted_factors.shape
    virtuals, _, pairs = amplitudes.shape
    window = window_rows.shape[0]
    out_index = lax.axis_index(OUT)
    con_index = lax.axis_index(CON)
    core = lax.axis_index("core").astype(jnp.int32)
    outs, cons = lax.axis_size(OUT), lax.axis_size(CON)
    groups = cons // 2
    half = window * block_d // outs
    parts = block_d // half
    c_half = parts * groups * half
    own_pairs = pairs // cons

    owned = select_rows(window_rows, out_index.astype(jnp.int32)[None], fitted_factors)
    tiles = lax.all_to_all(owned.reshape(outs, half, aux), OUT, 0, 0, tiled=True)
    piece = jnp.sum(tiles.astype(f32), axis=0).astype(bf16)
    piece, factors = lax.optimization_barrier((piece, fitted_factors))
    piece, amplitudes = lax.optimization_barrier((piece, amplitudes))
    rows = copy_for_each(piece, CHIPS)
    rows = rows.reshape(window * c_half, aux)

    f_own = factors.transpose(1, 0, 2)
    f_other = swap_cores(f_own)
    t_all = amplitudes.reshape(groups, 2, parts, half, block_d, pairs)
    t_all = t_all.transpose(1, 4, 2, 0, 3, 5).reshape(2, block_d, c_half, pairs)
    t_other = swap_cores(t_all)

    width = window * block_b
    old = old_rows(window_rows, amplitudes).reshape(groups, 2, own_pairs, window * block_d)

    rows, f_own, t_all, old = lax.optimization_barrier((rows, f_own, t_all, old))

    vectors = window_vectors(
        window_rows, core[None], rows.reshape(window, parts, groups, half, aux), block_d
    ).astype(bf16)
    sent = window_blocks(vectors, swap_cores(vectors), f_own, old)
    sent, rows = lax.optimization_barrier((sent, rows))
    got = lax.all_to_all(sent, CON[:-1], 0, 0, tiled=True)

    ladder = ladder_sums(core[None], rows, f_own, f_other, t_all, t_other, window)
    ladder, got, driver_term, occ_energy, vir_energy = lax.optimization_barrier(
        (ladder, got, driver_term, occ_energy, vir_energy)
    )
    tiles = lax.all_to_all(ladder.reshape(cons, own_pairs, width), CON, 0, 0, tiled=True)

    mask = window_rows[:, None] == jnp.arange(virtuals, dtype=jnp.int32)[None, :]
    window_energy = jnp.sum(jnp.where(mask, vir_energy[None, :], 0.0), axis=1)
    local_energy = lax.dynamic_slice_in_dim(vir_energy, out_index * block_b, block_b, 0)
    pair_energy = (occ_energy[:, None] + occ_energy[None, :]).reshape(-1)
    pair_energy = lax.dynamic_slice_in_dim(pair_energy, con_index * own_pairs, own_pairs, 0)
    denom = (window_energy[:, None] + local_energy[None, :]).reshape(1, -1) - pair_energy[:, None]
    driver = lax.dynamic_slice_in_dim(driver_term, con_index * own_pairs, own_pairs, 1)
    driver = driver.transpose(1, 0, 2).reshape(own_pairs, width)

    ladder_own, first_wide, first_own = first_step(tiles, driver, denom, window, outs)
    first_all = lax.all_to_all(first_wide, OUT, 0, 0, tiled=True)

    second_own = second_step(
        core[None], first_all, got, swap_cores(got), ladder_own, driver, denom, window
    )
    return (first_own, second_own)


def solution(mesh):
    fine = Mesh(mesh.devices.reshape(FINE), OUT + CON)
    return jax.shard_map(
        update,
        mesh=fine,
        in_specs=(P(OUT, CON, None), P(None, CON, None), P(None, None, OUT), P(), P(), P()),
        out_specs=(P(None, CON, OUT), P(None, CON, OUT)),
        check_vma=False,
    )
```

```python
import jax
import jax.numpy as jnp
from jax import lax
from jax.experimental import pallas as pl
from jax.experimental.pallas import tpu as pltpu
from jax.sharding import Mesh, PartitionSpec as P


OUT = ("x", "yl")
CON = ("z", "yh", "core")
CHIPS = ("x", "yl", "z", "yh")
FINE = (4, 2, 4, 2, 2)
D_STEP = 8
f32, bf16 = jnp.float32, jnp.bfloat16


def copy_for_each(value, axis):
    size = lax.axis_size(axis)
    return lax.all_to_all(
        jnp.broadcast_to(value[None], (size, *value.shape)), axis, 0, 0, tiled=True
    )


def swap_cores(value):
    return lax.ppermute(value, "core", [(0, 1), (1, 0)])


def in_vmem(*values):
    return [pltpu.with_memory_space_constraint(v, pltpu.VMEM) for v in values]


def dot_t(a, b):
    return lax.dot_general(a, b, (((1,), (1,)), ((), ())), preferred_element_type=f32)


def select_rows(window_rows, out_index, factors):
    window = window_rows.shape[0]
    block_b, block_d, aux = factors.shape

    def body(w_ref, o_index, *refs):
        for k in range(window):
            row = w_ref[k] - o_index[0] * block_b
            mine = (row >= 0) & (row < block_b)
            refs[-1][k] = jnp.where(mine, refs[k][0], jnp.zeros_like(refs[k][0]))

    def at(k):
        def row_map(i, w_ref, o_index):
            return (jnp.clip(w_ref[k] - o_index[0] * block_b, 0, block_b - 1), 0, 0)

        return pl.BlockSpec((1, block_d, aux), row_map)

    return pl.pallas_call(
        body,
        grid_spec=pltpu.PrefetchScalarGridSpec(
            num_scalar_prefetch=2,
            grid=(1,),
            in_specs=[at(k) for k in range(window)],
            out_specs=pl.BlockSpec((window, block_d, aux), lambda i, w, o: (0, 0, 0)),
        ),
        out_shape=jax.ShapeDtypeStruct((window, block_d, aux), bf16),
        name="select_rows",
    )(window_rows, out_index, *([factors] * window))


def window_vectors(window_rows, core, rows, block_d):
    window = window_rows.shape[0]
    _, _, _, half, aux = rows.shape

    def body(w_ref, c_ref, rows_ref, o_ref):
        picked = []
        for m in range(window):
            c = w_ref[m]
            mine = (c // block_d) % 2 == c_ref[0]
            r = lax.broadcasted_iota(jnp.int32, (half, aux), 0)
            keep = (r == c % half) & mine
            for k in range(window):
                tile = rows_ref[k, (c % block_d) // half, c // (2 * block_d)].astype(f32)
                row = jnp.sum(jnp.where(keep, tile, 0.0), axis=0, keepdims=True)
                picked.append(row)
        order = [picked[m * window + k] for k in range(window) for m in range(window)]
        o_ref[...] = jnp.concatenate(order, axis=0).astype(bf16)

    return pl.pallas_call(
        body,
        in_specs=[pl.BlockSpec(memory_space=pltpu.SMEM)] * 2
        + [pl.BlockSpec(memory_space=pltpu.VMEM)],
        out_specs=pl.BlockSpec(memory_space=pltpu.VMEM),
        out_shape=jax.ShapeDtypeStruct((window * window, aux), bf16),
        name="window_vectors",
    )(window_rows, core, *in_vmem(rows))


def window_blocks(vectors, more, factors, old):
    n, aux = vectors.shape
    block_d, block_b, _ = factors.shape
    chips, cores, own_pairs, count = old.shape
    window = count // block_d
    width = window * block_b
    tail = own_pairs * count // width
    steps = block_d // D_STEP

    def body(v_ref, u_ref, f_ref, p_ref, o_ref, w_ref):
        v = v_ref[...] + u_ref[...]
        v = jnp.concatenate([v, jnp.zeros((128 - n, aux), v.dtype)])
        x = dot_t(f_ref[...].reshape(-1, aux), v).T[:n]
        i = pl.program_id(0)
        for s in range(steps):

            @pl.when(i == s)
            def _():
                for d in range(D_STEP):
                    y = x[:, d * block_b : (d + 1) * block_b]
                    for h in range(width // 128):
                        w_ref[pl.ds(h * count + s * D_STEP + d, window, stride=block_d), :] = (
                            jnp.concatenate(
                                [
                                    y[k * window : (k + 1) * window]
                                    for k in range(h * 128 // block_b, (h + 1) * 128 // block_b)
                                ],
                                axis=1,
                            )
                        )

        @pl.when(i == steps - 1)
        def _():
            for h in range(width // 128):
                w = w_ref[h * count : (h + 1) * count].astype(bf16)
                for j in range(chips):
                    o_ref[j, :count, h * 128 : (h + 1) * 128] = w
            for h in range(cores):
                at = count + h * tail
                for j in range(width // count):
                    o_ref[:, at : at + tail, j * count : (j + 1) * count] = p_ref[
                        :, h, j * tail : (j + 1) * tail, :
                    ]

    return pl.pallas_call(
        body,
        grid=(steps,),
        in_specs=[
            pl.BlockSpec(memory_space=pltpu.VMEM),
            pl.BlockSpec(memory_space=pltpu.VMEM),
            pl.BlockSpec((D_STEP, block_b, aux), lambda i: (i, 0, 0)),
            pl.BlockSpec(old.shape, lambda i: (0, 0, 0, 0)),
        ],
        out_specs=pl.BlockSpec((chips, count + cores * tail, width), lambda i: (0, 0, 0)),
        out_shape=jax.ShapeDtypeStruct((chips, count + cores * tail, width), bf16),
        scratch_shapes=[pltpu.VMEM((width // 128 * count, 128), f32)],
        name="window_blocks",
    )(*in_vmem(vectors, more), factors, old)


def old_rows(window_rows, amplitudes):
    window = window_rows.shape[0]
    _, block_d, pairs = amplitudes.shape

    def body(*refs):
        x = jnp.concatenate([r[0].astype(f32) for r in refs[1:-1]], axis=0)
        refs[-1][...] = x.T.astype(bf16)

    def at(m):
        return pl.BlockSpec((1, block_d, pairs), lambda i, w: (w[m], 0, 0))

    return pl.pallas_call(
        body,
        grid_spec=pltpu.PrefetchScalarGridSpec(
            num_scalar_prefetch=1,
            grid=(1,),
            in_specs=[at(m) for m in range(window)],
            out_specs=pl.BlockSpec((pairs, window * block_d), lambda i, w: (0, 0)),
        ),
        out_shape=jax.ShapeDtypeStruct((pairs, window * block_d), bf16),
        name="old_rows",
    )(window_rows, *([amplitudes] * window))


def ladder_sums(core, rows, f_own, f_other, t_all, t_other, window):
    count, aux = rows.shape
    block_d, block_b, _ = f_own.shape
    _, _, c_half, pairs = t_all.shape
    steps = block_d // D_STEP

    def body(core_ref, a_ref, f1_ref, f2_ref, t1_ref, t2_ref, o_ref, lhs_ref, acc_ref):
        i = pl.program_id(0)

        @pl.when(i == 0)
        def _():
            acc_ref[...] = jnp.zeros_like(acc_ref)

        def step(f, t):
            for k in range(window):
                p = dot_t(f, a_ref[k * c_half : (k + 1) * c_half, :]).astype(bf16)
                for d in range(D_STEP):
                    lhs_ref[k * block_b : (k + 1) * block_b, d * c_half : (d + 1) * c_half] = p[
                        d * block_b : (d + 1) * block_b, :
                    ]
            acc_ref[...] += jnp.dot(lhs_ref[...], t, preferred_element_type=f32)

        @pl.when(i < steps)
        def _():
            step(f1_ref[...].reshape(-1, aux), t1_ref[...].reshape(-1, pairs))

        @pl.when(i >= steps)
        def _():
            step(f2_ref[...].reshape(-1, aux), t2_ref[...].reshape(-1, pairs))

        @pl.when(i == 2 * steps - 1)
        def _():
            o_ref[...] = acc_ref[...].T

    def first(i):
        return jnp.minimum(i, steps - 1)

    def second(i):
        return jnp.maximum(i - steps, 0)

    flops = 2 * 2 * block_d * block_b * count * (aux + pairs)
    return pl.pallas_call(
        body,
        grid_spec=pltpu.PrefetchScalarGridSpec(
            num_scalar_prefetch=1,
            grid=(2 * steps,),
            in_specs=[
                pl.BlockSpec((count, aux), lambda i, c: (0, 0)),
                pl.BlockSpec((D_STEP, block_b, aux), lambda i, c: (first(i), 0, 0)),
                pl.BlockSpec((D_STEP, block_b, aux), lambda i, c: (second(i), 0, 0)),
                pl.BlockSpec((1, D_STEP, c_half, pairs), lambda i, c: (c[0], first(i), 0, 0)),
                pl.BlockSpec((1, D_STEP, c_half, pairs), lambda i, c: (c[0], second(i), 0, 0)),
            ],
            out_specs=pl.BlockSpec((pairs, window * block_b), lambda i, c: (0, 0)),
            scratch_shapes=[
                pltpu.VMEM((window * block_b, D_STEP * c_half), bf16),
                pltpu.VMEM((window * block_b, pairs), f32),
            ],
        ),
        out_shape=jax.ShapeDtypeStruct((pairs, window * block_b), f32),
        cost_estimate=pl.CostEstimate(flops=flops, bytes_accessed=24_000_000, transcendentals=0),
        name="ladder_sums",
    )(core, rows, f_own, f_other, t_all, t_other)


def first_step(tiles, driver, denom, window, outs):
    _, own_pairs, width = tiles.shape
    block_b = width // window

    def body(t_ref, d_ref, e_ref, l_ref, w_ref, o_ref):
        ladder = jnp.sum(t_ref[...], axis=0)
        l_ref[...] = ladder
        value = ((d_ref[...] + ladder) / e_ref[...]).astype(bf16)
        for o in range(outs):
            w_ref[o] = value
        for k in range(window):
            o_ref[k] = value[:, k * block_b : (k + 1) * block_b]

    return pl.pallas_call(
        body,
        in_specs=[pl.BlockSpec(memory_space=pltpu.VMEM)] * 3,
        out_specs=[pl.BlockSpec(memory_space=pltpu.VMEM)] * 3,
        out_shape=(
            jax.ShapeDtypeStruct((own_pairs, width), f32),
            jax.ShapeDtypeStruct((outs, own_pairs, width), bf16),
            jax.ShapeDtypeStruct((window, own_pairs, block_b), bf16),
        ),
        name="first_step",
    )(*in_vmem(tiles, driver, denom))


def second_step(core, first_all, blocks, other, ladder, driver, denom, window):
    outs, own_pairs, width = first_all.shape
    block_b = width // window
    block_d = block_b // 2
    count = window * block_d
    tail = own_pairs * count // width

    def body(c_ref, f_ref, w_ref, x_ref, l_ref, d_ref, e_ref, o_ref, s_ref):
        total = l_ref[...]
        south = c_ref[0] == 0
        for o in range(outs):
            mine, theirs = w_ref[o, :count, :], x_ref[o, :count, :]
            halves = (jnp.where(south, mine, theirs), jnp.where(south, theirs, mine))
            olds = []
            for ref in (w_ref, x_ref):
                t = jnp.where(
                    south, ref[o, count : count + tail, :], ref[o, count + tail :, :]
                ).astype(f32)
                olds.append(
                    jnp.concatenate(
                        [t[:, j * count : (j + 1) * count] for j in range(width // count)], axis=0
                    )
                )
            olds = (jnp.where(south, olds[0], olds[1]), jnp.where(south, olds[1], olds[0]))
            old = jnp.concatenate(
                [
                    olds[h][:, m * block_d : (m + 1) * block_d]
                    for m in range(window)
                    for h in range(2)
                ],
                axis=1,
            )
            delta = (f_ref[o].astype(f32) - old).astype(bf16)
            for m in range(window):
                for h in range(2):
                    at = m * block_b + h * block_d
                    s_ref[at : at + block_d, :] = halves[h][m * block_d : (m + 1) * block_d, :]
            total = total + jnp.dot(delta, s_ref[...], preferred_element_type=f32)
        value = ((d_ref[...] + total) / e_ref[...]).astype(bf16)
        for k in range(window):
            o_ref[k] = value[:, k * block_b : (k + 1) * block_b]

    return pl.pallas_call(
        body,
        in_specs=[pl.BlockSpec(memory_space=pltpu.SMEM)]
        + [pl.BlockSpec(memory_space=pltpu.VMEM)] * 6,
        out_specs=pl.BlockSpec(memory_space=pltpu.VMEM),
        out_shape=jax.ShapeDtypeStruct((window, own_pairs, block_b), bf16),
        scratch_shapes=[pltpu.VMEM((width, width), bf16)],
        name="second_step",
    )(core, *in_vmem(first_all, blocks, other, ladder, driver, denom))


def update(fitted_factors, amplitudes, driver_term, occ_energy, vir_energy, window_rows):
    block_b, block_d, aux = fitted_factors.shape
    virtuals, _, pairs = amplitudes.shape
    window = window_rows.shape[0]
    out_index = lax.axis_index(OUT)
    con_index = lax.axis_index(CON)
    core = lax.axis_index("core").astype(jnp.int32)
    outs, cons = lax.axis_size(OUT), lax.axis_size(CON)
    groups = cons // 2
    half = window * block_d // outs
    parts = block_d // half
    c_half = parts * groups * half
    own_pairs = pairs // cons

    owned = select_rows(window_rows, out_index.astype(jnp.int32)[None], fitted_factors)
    tiles = lax.all_to_all(owned.reshape(outs, half, aux), OUT, 0, 0, tiled=True)
    piece = jnp.sum(tiles.astype(f32), axis=0).astype(bf16)
    piece, factors = lax.optimization_barrier((piece, fitted_factors))
    piece, amplitudes = lax.optimization_barrier((piece, amplitudes))
    rows = copy_for_each(piece, CHIPS)
    rows = rows.reshape(window * c_half, aux)

    f_own = factors.transpose(1, 0, 2)
    f_other = swap_cores(f_own)
    t_all = amplitudes.reshape(groups, 2, parts, half, block_d, pairs)
    t_all = t_all.transpose(1, 4, 2, 0, 3, 5).reshape(2, block_d, c_half, pairs)
    t_other = swap_cores(t_all)

    width = window * block_b
    old = old_rows(window_rows, amplitudes).reshape(groups, 2, own_pairs, window * block_d)

    rows, f_own, t_all, old = lax.optimization_barrier((rows, f_own, t_all, old))

    vectors = window_vectors(
        window_rows, core[None], rows.reshape(window, parts, groups, half, aux), block_d
    )
    sent = window_blocks(vectors, swap_cores(vectors), f_own, old)
    sent, rows = lax.optimization_barrier((sent, rows))
    got = lax.all_to_all(sent, CON[:-1], 0, 0, tiled=True)

    ladder = ladder_sums(core[None], rows, f_own, f_other, t_all, t_other, window)
    ladder, got, driver_term, occ_energy, vir_energy = lax.optimization_barrier(
        (ladder, got, driver_term, occ_energy, vir_energy)
    )
    tiles = lax.all_to_all(ladder.reshape(cons, own_pairs, width), CON, 0, 0, tiled=True)

    mask = window_rows[:, None] == jnp.arange(virtuals, dtype=jnp.int32)[None, :]
    window_energy = jnp.sum(jnp.where(mask, vir_energy[None, :], 0.0), axis=1)
    local_energy = lax.dynamic_slice_in_dim(vir_energy, out_index * block_b, block_b, 0)
    pair_energy = (occ_energy[:, None] + occ_energy[None, :]).reshape(-1)
    pair_energy = lax.dynamic_slice_in_dim(pair_energy, con_index * own_pairs, own_pairs, 0)
    denom = (window_energy[:, None] + local_energy[None, :]).reshape(1, -1) - pair_energy[:, None]
    driver = lax.dynamic_slice_in_dim(driver_term, con_index * own_pairs, own_pairs, 1)
    driver = driver.transpose(1, 0, 2).reshape(own_pairs, width)

    ladder_own, first_wide, first_own = first_step(tiles, driver, denom, window, outs)
    first_all = lax.all_to_all(first_wide, OUT, 0, 0, tiled=True)

    second_own = second_step(
        core[None], first_all, got, swap_cores(got), ladder_own, driver, denom, window
    )
    return (first_own, second_own)


def solution(mesh):
    fine = Mesh(mesh.devices.reshape(FINE), OUT + CON)
    return jax.shard_map(
        update,
        mesh=fine,
        in_specs=(P(OUT, CON, None), P(None, CON, None), P(None, None, OUT), P(), P(), P()),
        out_specs=(P(None, CON, OUT), P(None, CON, OUT)),
        check_vma=False,
    )
```
